32 devices in a mesh: seq: 32 (over z, y, x, core).
Axes of the slice: x: 2, y: 2, z: 4, core: 2. Of those that a mesh axis runs over, the one named last changes fastest.
Arguments:
- inputs: bfloat16 [4096, 4096], P('seq'), may hold values from -6 to 6
- step_sizes: bfloat16 [4096, 4096], P('seq'), may hold values from 0.25 to 2
- cotangent: bfloat16 [4096, 4096], P('seq'), may hold values from -6 to 6
- input_coeffs: float32 [16, 4096], P(None, 'seq'), may hold values from -0.3 to 0.3
- output_coeffs: float32 [16, 4096], P(None, 'seq'), may hold values from -0.3 to 0.3
- decay_rates: float32 [16, 4096], replicated, as said below
Outputs:
- grad_inputs: bfloat16 [4096, 4096], P('seq')
- grad_steps: bfloat16 [4096, 4096], P('seq')
- grad_in_coeffs: float32 [16, 4096], P(None, 'seq')
- grad_out_coeffs: float32 [16, 4096], P(None, 'seq')
- grad_rates: float32 [16, 4096], P(None, 'seq')
The draws below stay inside these ranges and needn't reach their ends.
Inputs may be any that keep to these rules, and one draw needn't show every extreme that they name: `decay_rates`: every entry lies between 0.1 / 4096 and 0.15.
All inputs are finite; a program needn't handle non-finite values.
Results may differ from the reference program's by a relative error of at most 0.001.
Values sent between devices are 32-bit elements; how exact they have to be, the bound alone decides.
A program may use at most 64 MiB of HBM per device.

```python
import math
from functools import partial
import jax
import jax.numpy as jnp
from jax import lax

CHANNELS = 4096
STATE = 16
TOK_DEV = 128
TOKENS = 4096


def draw_decay_rates(key, part):
    chooser_key, slow_key, fast_key = jax.random.split(jax.random.fold_in(key, 7), 3)
    chooser = jax.random.uniform(chooser_key, (CHANNELS,), jnp.float32)
    fast_rates = jnp.exp(jax.random.uniform(fast_key, (STATE, CHANNELS), jnp.float32, math.log(0.05), math.log(0.15)))
    slow_share = 0.5
    slow_rates = jnp.exp(jax.random.uniform(slow_key, (STATE, CHANNELS), jnp.float32, math.log(0.3), 0.0)) / TOK_DEV
    return jnp.where(chooser[None, :] < slow_share, slow_rates, fast_rates).astype(jnp.float32)


def draw_step_sizes(key, part):
    level_key, jitter_key = jax.random.split(jax.random.fold_in(key, 11), 2)
    run_count = TOKENS // 128
    levels = jax.random.uniform(level_key, (run_count, 1, CHANNELS), jnp.float32, -0.6, 1.2)
    jitter = jax.random.uniform(jitter_key, (run_count, 128, CHANNELS), jnp.float32, -0.5, 0.5)
    values = jnp.clip(0.5 * jnp.exp(levels + jitter), 0.25, 2.0)
    return values.reshape(TOKENS, CHANNELS).astype(jnp.bfloat16)


def block_levels(rng, shape, cuts, least, top_value):
    loudness, own = 1.0, jax.random.fold_in(rng, 6)
    for axis_at, shards_of in cuts:
        heights = jnp.exp(jax.random.uniform(jax.random.fold_in(own, axis_at), (shards_of,), jnp.float32, least / len(cuts), top_value / len(cuts)))
        loudness = loudness * jnp.repeat(heights, shape[axis_at] // shards_of).reshape([-1 if axis == axis_at else 1 for axis in range(len(shape))])
    return loudness


def scatter_about(rng, extent, deviation, reach, cuts=(), dtype=jnp.bfloat16):
    entries = deviation * jax.random.normal(rng, extent, jnp.float32)
    if cuts:
        entries = entries * block_levels(rng, extent, cuts, -0.22, 0.18)
    return jnp.clip(entries, -reach, reach).astype(dtype)


def setup_inputs(seed: int = 0) -> dict:
    key_list = jax.random.split(jax.random.key(seed), 7)
    inputs = scatter_about(key_list[0], (TOKENS, CHANNELS), 1.0, 6.0, ((0, 32),))
    step_sizes = draw_step_sizes(jax.random.fold_in(key_list[6], 71), 0)
    cotangent = scatter_about(key_list[2], (TOKENS, CHANNELS), 1.0, 6.0, ((0, 32),))
    input_coeffs = scatter_about(key_list[3], (STATE, TOKENS), 0.05, 0.3, ((1, 32),), jnp.float32)
    output_coeffs = scatter_about(key_list[4], (STATE, TOKENS), 0.05, 0.3, ((1, 32),), jnp.float32)
    decay_rates = draw_decay_rates(jax.random.fold_in(key_list[6], 71), 0)
    return {"inputs": inputs, "step_sizes": step_sizes, "cotangent": cotangent, "input_coeffs": input_coeffs, "output_coeffs": output_coeffs, "decay_rates": decay_rates}


block_len = 32


def blocked(array):
    return array.reshape(array.shape[0] // block_len, block_len, array.shape[1])


def sweep_forward(initial, inputs, step_sizes, in_rows, decay_rates):
    def per_block(hidden, block_data):
        block_input, block_delta, block_bcoef = block_data
        anchor = hidden
        for position in range(block_len):
            row_delta = block_delta[position].astype(jnp.float32)
            decay_row = jnp.exp(-row_delta[None, :] * decay_rates)
            drive = block_bcoef[position][:, None] * (row_delta * block_input[position].astype(jnp.float32))[None, :]
            hidden = decay_row * hidden + drive
        return hidden, anchor
    return lax.scan(per_block, initial, (blocked(inputs), blocked(step_sizes), blocked(in_rows)))


def block_grads(carried, block_data, decay_rates):
    later, grad_rates = carried
    anchor, block_input, block_delta, block_bcoef, block_ccoef, block_grad = block_data
    hidden_list = [anchor]
    for position in range(block_len):
        row_delta = block_delta[position].astype(jnp.float32)
        decay_row = jnp.exp(-row_delta[None, :] * decay_rates)
        drive = block_bcoef[position][:, None] * (row_delta * block_input[position].astype(jnp.float32))[None, :]
        hidden_list.append(decay_row * hidden_list[-1] + drive)
    input_rows = [None] * block_len
    step_rows = [None] * block_len
    bcoef_rows = [None] * block_len
    ccoef_rows = [None] * block_len
    for position in reversed(range(block_len)):
        row_delta = block_delta[position].astype(jnp.float32)
        row_input = block_input[position].astype(jnp.float32)
        row_grad = block_grad[position].astype(jnp.float32)
        decay_row = jnp.exp(-row_delta[None, :] * decay_rates)
        grad_state = block_ccoef[position][:, None] * row_grad[None, :] + later
        coeff_sum = jnp.sum(grad_state * block_bcoef[position][:, None], 0)
        weighted = grad_state * decay_row * hidden_list[position]
        input_rows[position] = (row_delta * coeff_sum).astype(jnp.bfloat16)
        step_rows[position] = (row_input * coeff_sum - jnp.sum(weighted * decay_rates, 0)).astype(jnp.bfloat16)
        bcoef_rows[position] = jnp.sum(grad_state * (row_delta * row_input)[None, :], 1)
        ccoef_rows[position] = jnp.sum(hidden_list[position + 1] * row_grad[None, :], 1)
        grad_rates = grad_rates - weighted * row_delta[None, :]
        later = decay_row * grad_state
    return (later, grad_rates), (jnp.stack(input_rows), jnp.stack(step_rows), jnp.stack(bcoef_rows), jnp.stack(ccoef_rows))


def reference(inputs, step_sizes, cotangent, input_coeffs, output_coeffs, decay_rates):
    blank = jnp.zeros(decay_rates.shape, jnp.float32)
    in_rows = input_coeffs.T
    out_rows = output_coeffs.T
    _, anchors = sweep_forward(blank, inputs, step_sizes, in_rows, decay_rates)
    block_data = (anchors, blocked(inputs), blocked(step_sizes), blocked(in_rows), blocked(out_rows), blocked(cotangent))
    (_, grad_rates), pieces = lax.scan(partial(block_grads, decay_rates=decay_rates), (blank, blank), block_data, reverse=True)
    channels = inputs.shape[1]
    n_state = decay_rates.shape[0]
    grad_inputs = pieces[0].reshape(-1, channels)
    grad_steps = pieces[1].reshape(-1, channels)
    grad_in_coeffs = pieces[2].reshape(-1, n_state).T
    grad_out_coeffs = pieces[3].reshape(-1, n_state).T
    return (grad_inputs, grad_steps, grad_in_coeffs, grad_out_coeffs, grad_rates)
```

```python
from functools import partial
import math

import jax
import jax.numpy as jnp
from jax import lax
from jax.experimental import pallas as pl
from jax.experimental.pallas import tpu as pltpu
from jax.sharding import PartitionSpec as P

LANES = 128
SUB = 8
TILES = 4
GROUP = 8
LOG2E = math.log2(math.e)
LN2 = math.log(2.0)
F32 = jnp.float32
MESH = pl.DeviceIdType.MESH


def expand(coef_ref, wide, tokens, n_state):
    for t in range(tokens):
        wide[t] = jnp.broadcast_to(coef_ref[:, t : t + 1], (n_state, LANES))


def row(ref, k, t):
    return ref[k, pl.ds(t, SUB, stride=0), :]


def lanes_of(k):
    return slice(k * LANES, (k + 1) * LANES)


def part(h):
    return slice(h * SUB, (h + 1) * SUB)


def summary_kernel(x_ref, d_ref, g_ref, b_ref, c_ref, a_ref, out_ref, bx, cx, dl, uu, gg, st):
    tokens, block = x_ref.shape
    n_state = a_ref.shape[0]
    halves, tiles = n_state // SUB, block // LANES

    @pl.when(pl.program_id(0) == 0)
    def _():
        expand(b_ref, bx, tokens, n_state)
        expand(c_ref, cx, tokens, n_state)

    for k in range(tiles):
        delta = d_ref[:, lanes_of(k)].astype(F32)
        dl[k] = delta
        uu[k] = delta * x_ref[:, lanes_of(k)].astype(F32)
        gg[k] = g_ref[:, lanes_of(k)].astype(F32)
    rates = [[a_ref[part(h), lanes_of(k)] * (-LOG2E) for h in range(halves)] for k in range(tiles)]

    def group(i, carry):
        prod, end, back = [[list(c) for c in v] for v in carry]
        for s in range(GROUP):
            t = i * GROUP + s
            bs = [bx[t, part(h), :] for h in range(halves)]
            cs = [cx[t, part(h), :] for h in range(halves)]
            for k in range(tiles):
                delta, u, g = row(dl, k, t), row(uu, k, t), row(gg, k, t)
                for h in range(halves):
                    decay = jnp.exp2(delta * rates[k][h])
                    end[k][h] = decay * end[k][h] + bs[h] * u
                    prod[k][h] = decay * prod[k][h]
                    back[k][h] = back[k][h] + prod[k][h] * (cs[h] * g)
        return prod, end, back

    ones = [[jnp.ones((SUB, LANES), F32)] * halves for _ in range(tiles)]
    zeros = [[jnp.zeros((SUB, LANES), F32)] * halves for _ in range(tiles)]
    results = lax.fori_loop(0, tokens // GROUP, group, (ones, zeros, zeros))
    for v in range(3):
        for k in range(tiles):
            for h in range(halves):
                st[v * n_state + h * SUB : v * n_state + (h + 1) * SUB, lanes_of(k)] = results[v][k][h]
    width = out_ref.shape[2]
    for j in range(block // width):
        out_ref[j] = st[:, j * width : (j + 1) * width]


def greet_all(me, n):
    barrier = pltpu.get_barrier_semaphore()

    def tell(k, _):
        pl.semaphore_signal(barrier, inc=1, device_id=(lax.rem(me + k, n),), device_id_type=MESH)
        return 0

    lax.fori_loop(1, n, tell, 0)
    pl.semaphore_wait(barrier, n - 1)


def exchange_copy(me, n, k, src, dst, send_sem, recv_sem):
    dest = lax.rem(me + k, n)
    return pltpu.make_async_remote_copy(
        src_ref=src.at[dest],
        dst_ref=dst.at[me],
        send_sem=send_sem.at[k],
        recv_sem=recv_sem.at[me],
        device_id=(dest,),
        device_id_type=MESH,
    )


def arrival(me, n, k, src, dst, send_sem, recv_sem):
    origin = lax.rem(me + n - k, n)
    return pltpu.make_async_remote_copy(
        src_ref=src.at[origin],
        dst_ref=dst.at[origin],
        send_sem=send_sem.at[k],
        recv_sem=recv_sem.at[origin],
        device_id=(origin,),
        device_id_type=MESH,
    )


def loop(n, body):
    def step(k, _):
        body(k)
        return 0

    lax.fori_loop(1, n, step, 0)


def chain_kernel(n, send_ref, out_ref, recv, back, send1, recv1, send2, recv2):
    me = lax.axis_index("seq")
    n_state = send_ref.shape[1] // 3
    width = send_ref.shape[2]
    greet_all(me, n)
    first = (send_ref, recv, send1, recv1)
    second = (back, out_ref, send2, recv2)
    loop(n, lambda k: exchange_copy(me, n, k, *first).start())
    recv[me] = send_ref[me]
    loop(n, lambda k: arrival(me, n, k, *first).wait_recv())

    def ahead(d, value):
        back[d, :n_state, :] = value
        return recv[d, :n_state, :] * value + recv[d, n_state : 2 * n_state, :]

    def behind(i, value):
        d = n - 1 - i
        back[d, n_state:, :] = value
        return recv[d, :n_state, :] * value + recv[d, 2 * n_state :, :]

    blank = jnp.zeros((n_state, width), F32)
    lax.fori_loop(0, n, ahead, blank)
    lax.fori_loop(0, n, behind, blank)
    loop(n, lambda k: exchange_copy(me, n, k, *second).start())
    out_ref[me] = back[me]
    loop(n, lambda k: arrival(me, n, k, *second).wait_recv())
    loop(n, lambda k: exchange_copy(me, n, k, *first).wait_send())
    loop(n, lambda k: exchange_copy(me, n, k, *second).wait_send())


def total_kernel(n, send_ref, out_ref, recv, send1, recv1):
    me = lax.axis_index("seq")
    greet_all(me, n)
    refs = (send_ref, recv, send1, recv1)
    loop(n, lambda k: exchange_copy(me, n, k, *refs).start())
    recv[me] = send_ref[me]
    loop(n, lambda k: arrival(me, n, k, *refs).wait_recv())
    out_ref[...] = lax.fori_loop(
        0, n, lambda d, total: total + recv[d], jnp.zeros(out_ref.shape, F32)
    )
    loop(n, lambda k: exchange_copy(me, n, k, *refs).wait_send())


def lane_sums(acc, out_ref, tokens, n_state):
    lane = lax.broadcasted_iota(jnp.int32, (n_state, tokens), 1)
    total = jnp.zeros((n_state, tokens), F32)
    for t in range(tokens):
        total = jnp.where(lane == t, jnp.sum(acc[t], axis=1, keepdims=True), total)
    out_ref[...] = total


def grads_kernel(
    x_ref, d_ref, g_ref, b_ref, c_ref, a_ref, edge_ref,
    gi_ref, gs_ref, gb_ref, gc_ref, gr_ref,
    bx, cx, dl, xx, uu, gg, st, hs, dec, accb, accc, csp, awp, gi, gs,
):
    tokens, block = x_ref.shape
    n_state = a_ref.shape[0]
    halves, tiles = n_state // SUB, block // LANES
    width = edge_ref.shape[2]

    @pl.when(pl.program_id(0) == 0)
    def _():
        expand(b_ref, bx, tokens, n_state)
        expand(c_ref, cx, tokens, n_state)
        accb[...] = jnp.zeros_like(accb)
        accc[...] = jnp.zeros_like(accc)

    for k in range(tiles):
        delta = d_ref[:, lanes_of(k)].astype(F32)
        x = x_ref[:, lanes_of(k)].astype(F32)
        dl[k] = delta
        xx[k] = x
        uu[k] = delta * x
        gg[k] = g_ref[:, lanes_of(k)].astype(F32)
    for j in range(block // width):
        st[:, j * width : (j + 1) * width] = edge_ref[j]
    rates = [[a_ref[part(h), lanes_of(k)] * (-LOG2E) for h in range(halves)] for k in range(tiles)]

    def slot(k, h):
        return slice((k * halves + h) * SUB, (k * halves + h + 1) * SUB)

    def ahead(i, carry):
        hidden = [list(c) for c in carry]
        for s in range(GROUP):
            t = i * GROUP + s
            bs = [bx[t, part(h), :] for h in range(halves)]
            sums = [None] * halves
            for k in range(tiles):
                delta, u, g = row(dl, k, t), row(uu, k, t), row(gg, k, t)
                for h in range(halves):
                    decay = jnp.exp2(delta * rates[k][h])
                    dec[t, slot(k, h), :] = decay
                    hs[t, slot(k, h), :] = hidden[k][h]
                    hidden[k][h] = decay * hidden[k][h] + bs[h] * u
                    term = g * hidden[k][h]
                    sums[h] = term if sums[h] is None else sums[h] + term
            for h in range(halves):
                accc[t, part(h), :] += sums[h]
        return hidden

    start = [[st[part(h), lanes_of(k)] for h in range(halves)] for k in range(tiles)]
    lax.fori_loop(0, tokens // GROUP, ahead, start)

    def behind(i, carry):
        later, rate = [[list(c) for c in v] for v in carry]
        base = tokens - GROUP - i * GROUP
        for s in reversed(range(GROUP)):
            t = base + s
            bs = [bx[t, part(h), :] for h in range(halves)]
            cs = [cx[t, part(h), :] for h in range(halves)]
            sums = [None] * halves
            for k in range(tiles):
                delta, u, g = row(dl, k, t), row(uu, k, t), row(gg, k, t)
                coeff = weigh = None
                for h in range(halves):
                    state = cs[h] * g + later[k][h]
                    later[k][h] = dec[t, slot(k, h), :] * state
                    weighted = later[k][h] * hs[t, slot(k, h), :]
                    rate[k][h] = rate[k][h] + weighted * delta
                    one, two, three = state * bs[h], weighted * rates[k][h], state * u
                    coeff = one if coeff is None else coeff + one
                    weigh = two if weigh is None else weigh + two
                    sums[h] = three if sums[h] is None else sums[h] + three
                csp[k, part(s), :] = coeff
                awp[k, part(s), :] = weigh
            for h in range(halves):
                accb[t, part(h), :] += sums[h]
        rows = pl.ds(pl.multiple_of(base, GROUP), GROUP)
        for k in range(tiles):
            coeff = csp[k, pl.ds(0, GROUP, stride=SUB), :]
            weigh = awp[k, pl.ds(0, GROUP, stride=SUB), :]
            for s in range(1, SUB):
                coeff = coeff + csp[k, pl.ds(s, GROUP, stride=SUB), :]
                weigh = weigh + awp[k, pl.ds(s, GROUP, stride=SUB), :]
            gi[k, rows, :] = dl[k, rows, :] * coeff
            gs[k, rows, :] = xx[k, rows, :] * coeff + LN2 * weigh
        return later, rate

    last = [[st[n_state + h * SUB : n_state + (h + 1) * SUB, lanes_of(k)] for h in range(halves)] for k in range(tiles)]
    zeros = [[jnp.zeros((SUB, LANES), F32)] * halves for _ in range(tiles)]
    _, rate = lax.fori_loop(0, tokens // GROUP, behind, (last, zeros))
    for k in range(tiles):
        gi_ref[:, lanes_of(k)] = gi[k].astype(gi_ref.dtype)
        gs_ref[:, lanes_of(k)] = gs[k].astype(gs_ref.dtype)
        for h in range(halves):
            st[part(h), lanes_of(k)] = -rate[k][h]
    for j in range(block // width):
        gr_ref[j] = st[:n_state, j * width : (j + 1) * width]

    @pl.when(pl.program_id(0) == pl.num_programs(0) - 1)
    def _():
        lane_sums(accb, gb_ref, tokens, n_state)
        lane_sums(accc, gc_ref, tokens, n_state)


def shards(n, inputs, step_sizes, cotangent, input_coeffs, output_coeffs, decay_rates):
    n_state, channels = decay_rates.shape
    tokens = inputs.shape[0]
    width = channels // n
    block = max(TILES * LANES, width)
    tiles = block // LANES
    owners = block // width
    grid = (channels // block,)
    seq_spec = pl.BlockSpec((tokens, block), lambda i: (0, i))
    coef_spec = pl.BlockSpec((n_state, tokens), lambda i: (0, 0))
    rate_spec = pl.BlockSpec((n_state, block), lambda i: (0, i))
    own_spec = lambda rows: pl.BlockSpec((owners, rows, width), lambda i: (i, 0, 0))
    wide = pltpu.VMEM((tokens, n_state, LANES), F32)
    rows = pltpu.VMEM((tiles, tokens, LANES), F32)
    states = pltpu.VMEM((tokens, tiles * n_state, LANES), F32)
    fold = pltpu.VMEM((tiles, GROUP * SUB, LANES), F32)
    vmem = pl.BlockSpec(memory_space=pltpu.VMEM)
    dma = pltpu.SemaphoreType.DMA((n,))
    operands = (inputs, step_sizes, cotangent, input_coeffs, output_coeffs, decay_rates)
    operand_specs = [seq_spec] * 3 + [coef_spec] * 2 + [rate_spec]

    summary = pl.pallas_call(
        summary_kernel,
        name="summary",
        grid=grid,
        in_specs=operand_specs,
        out_specs=own_spec(3 * n_state),
        out_shape=jax.ShapeDtypeStruct((n, 3 * n_state, width), F32),
        scratch_shapes=[wide, wide, rows, rows, rows, pltpu.VMEM((3 * n_state, block), F32)],
        compiler_params=pltpu.CompilerParams(dimension_semantics=("arbitrary",)),
    )(*operands)

    edges = pl.pallas_call(
        partial(chain_kernel, n),
        name="chain",
        in_specs=[vmem],
        out_specs=vmem,
        out_shape=jax.ShapeDtypeStruct((n, 2 * n_state, width), F32),
        scratch_shapes=[
            pltpu.VMEM((n, 3 * n_state, width), F32),
            pltpu.VMEM((n, 2 * n_state, width), F32),
            dma, dma, dma, dma,
        ],
        compiler_params=pltpu.CompilerParams(collective_id=0, has_side_effects=True),
    )(summary)

    gi, gs, gb, gc, gr = pl.pallas_call(
        grads_kernel,
        name="grads",
        grid=grid,
        in_specs=operand_specs + [own_spec(2 * n_state)],
        out_specs=[seq_spec, seq_spec, coef_spec, coef_spec, own_spec(n_state)],
        out_shape=[
            jax.ShapeDtypeStruct((tokens, channels), jnp.bfloat16),
            jax.ShapeDtypeStruct((tokens, channels), jnp.bfloat16),
            jax.ShapeDtypeStruct((n_state, tokens), F32),
            jax.ShapeDtypeStruct((n_state, tokens), F32),
            jax.ShapeDtypeStruct((n, n_state, width), F32),
        ],
        scratch_shapes=[
            wide, wide, rows, rows, rows, rows,
            pltpu.VMEM((2 * n_state, block), F32),
            states, states, wide, wide, fold, fold, rows, rows,
        ],
        compiler_params=pltpu.CompilerParams(
            dimension_semantics=("arbitrary",), vmem_limit_bytes=48 * 1024 * 1024
        ),
    )(*operands, edges)

    grad_rates = pl.pallas_call(
        partial(total_kernel, n),
        name="total",
        in_specs=[vmem],
        out_specs=vmem,
        out_shape=jax.ShapeDtypeStruct((n_state, width), F32),
        scratch_shapes=[pltpu.VMEM((n, n_state, width), F32), dma, dma],
        compiler_params=pltpu.CompilerParams(collective_id=1, has_side_effects=True),
    )(gr)
    return gi, gs, gb, gc, grad_rates


def solution(mesh):
    placed = (P("seq", None), P("seq", None), P("seq", None), P(None, "seq"), P(None, "seq"), P())
    return jax.shard_map(
        partial(shards, mesh.shape["seq"]),
        mesh=mesh,
        in_specs=placed,
        out_specs=(P("seq", None), P("seq", None), P(None, "seq"), P(None, "seq"), P(None, "seq")),
        check_vma=False,
    )
```

```python
from functools import partial
import math

import jax
import jax.numpy as jnp
from jax import lax
from jax.experimental import pallas as pl
from jax.experimental.pallas import tpu as pltpu
from jax.sharding import PartitionSpec as P

LANES = 128
SUB = 8
TILES = 4
GROUP = 8
LOG2E = math.log2(math.e)
LN2 = math.log(2.0)
F32 = jnp.float32
MESH = pl.DeviceIdType.MESH


def expand(coef_ref, wide, tokens, n_state):
    for t in range(tokens):
        wide[t] = jnp.broadcast_to(coef_ref[:, t : t + 1], (n_state, LANES))


def row(ref, t, n_state):
    return ref[:, pl.ds(t, n_state, stride=0), :]


def lanes_of(k):
    return slice(k * LANES, (k + 1) * LANES)


def loop(start, stop, body):
    def step(k, _):
        body(k)
        return 0

    lax.fori_loop(start, stop, step, 0)


def lane_sums(acc, out_ref, tokens, n_state):
    lane = lax.broadcasted_iota(jnp.int32, (n_state, tokens), 1)
    total = jnp.zeros((n_state, tokens), F32)
    for t in range(tokens):
        total = jnp.where(lane == t, jnp.sum(acc[t], axis=1, keepdims=True), total)
    out_ref[...] = total


def whole_kernel(
    n, block,
    x_ref, d_ref, g_ref, b_ref, c_ref, a_ref,
    gi_ref, gs_ref, gb_ref, gc_ref, gr_ref,
    bx, cx, dl, xx, uu, gg, rt, st, hs, dec, accb, accc, csp, awp, gi, gs,
    out1, in1, out2, in2, out3, in3, send1, recv1, send2, recv2, send3, recv3,
):
    me = lax.axis_index("seq")
    tokens, channels = x_ref.shape
    n_state = a_ref.shape[0]
    tiles, width = block // LANES, channels // n
    blocks, owners = channels // block, block // width
    home = me // owners
    barrier = pltpu.get_barrier_semaphore()

    def tell(k):
        pl.semaphore_signal(barrier, inc=1, device_id=(lax.rem(me + k, n),), device_id_type=MESH)

    def copy(src, dst, send_sem, recv_sem, dest, slot):
        return pltpu.make_async_remote_copy(
            src_ref=src.at[dest],
            dst_ref=dst.at[slot],
            send_sem=send_sem.at[dest],
            recv_sem=recv_sem.at[slot],
            device_id=(dest,),
            device_id_type=MESH,
        )

    first = (out1, in1, send1, recv1)
    second = (out2, in2, send2, recv2)
    third = (out3, in3, send3, recv3)

    def stage(b):
        for k in range(tiles):
            lanes = pl.ds(pl.multiple_of(b * block + k * LANES, LANES), LANES)
            delta = d_ref[:, lanes].astype(F32)
            x = x_ref[:, lanes].astype(F32)
            dl[k] = delta
            xx[k] = x
            uu[k] = delta * x
            gg[k] = g_ref[:, lanes].astype(F32)
            rt[k] = a_ref[:, lanes] * (-LOG2E)

    loop(1, n, tell)
    expand(b_ref, bx, tokens, n_state)
    expand(c_ref, cx, tokens, n_state)
    accb[...] = jnp.zeros_like(accb)
    accc[...] = jnp.zeros_like(accc)
    state_shape = (tiles, n_state, LANES)

    def summarize(order):
        b = lax.rem(home + 1 + order, blocks)
        stage(b)
        rates = rt[...]

        def group(i, carry):
            prod, end, back = carry
            for s in range(GROUP):
                t = i * GROUP + s
                decay = jnp.exp2(row(dl, t, n_state) * rates)
                end = decay * end + bx[t][None] * row(uu, t, n_state)
                prod = decay * prod
                back = back + prod * (cx[t][None] * row(gg, t, n_state))
            return prod, end, back

        zero = jnp.zeros(state_shape, F32)
        _, end, back = lax.fori_loop(
            0, tokens // GROUP, group, (jnp.ones(state_shape, F32), zero, zero)
        )
        for k in range(tiles):
            st[:n_state, lanes_of(k)] = end[k]
            st[n_state : 2 * n_state, lanes_of(k)] = back[k]
            st[2 * n_state :, lanes_of(k)] = jnp.broadcast_to(
                jnp.sum(dl[k], axis=0, keepdims=True), (SUB, LANES)
            )

        @pl.when(order == 0)
        def _():
            pl.semaphore_wait(barrier, n - 1)

        for j in range(owners):
            dest = b * owners + j
            out1[dest] = st[:, j * width : (j + 1) * width]

            @pl.when(dest != me)
            def _():
                copy(*first, dest, me).start()

    loop(0, blocks, summarize)
    in1[me] = out1[me]

    def arrived(refs):
        def wait(k):
            origin = lax.rem(me + n - k, n)
            copy(*refs, origin, origin).wait_recv()

        loop(1, n, wait)

    arrived(first)
    if width % LANES == 0:
        own = a_ref[:, pl.ds(pl.multiple_of(me * width, LANES), width)] * (-LOG2E)
    else:
        own = jnp.zeros((n_state, width), F32)
        for j in range(n):
            own = jnp.where(me == j, a_ref[:, j * width : (j + 1) * width] * (-LOG2E), own)

    def scan(i, carry):
        ahead, behind = carry
        d, e = i, n - 1 - i
        out2[d, :n_state, :] = ahead
        out2[e, n_state:, :] = behind
        ahead = jnp.exp2(own * in1[d, 2 * n_state : 2 * n_state + 1, :]) * ahead + in1[d, :n_state, :]
        behind = (
            jnp.exp2(own * in1[e, 2 * n_state : 2 * n_state + 1, :]) * behind
            + in1[e, n_state : 2 * n_state, :]
        )
        return ahead, behind

    blank = jnp.zeros((n_state, width), F32)
    lax.fori_loop(0, n, scan, (blank, blank))
    loop(1, n, lambda k: copy(*second, lax.rem(me + n - k, n), me).start())
    in2[me] = out2[me]

    def differentiate(order, _):
        b = lax.rem(home + order, blocks)
        stage(b)
        for j in range(owners):
            origin = b * owners + j

            @pl.when(origin != me)
            def _():
                copy(*second, origin, origin).wait_recv()

            st[: 2 * n_state, j * width : (j + 1) * width] = in2[origin]
        rates = rt[...]

        def ahead(i, hidden):
            for s in range(GROUP):
                t = i * GROUP + s
                decay = jnp.exp2(row(dl, t, n_state) * rates)
                dec[t] = decay
                hs[t] = hidden
                hidden = decay * hidden + bx[t][None] * row(uu, t, n_state)
                accc[t] += jnp.sum(row(gg, t, n_state) * hidden, axis=0)
            return hidden

        start = jnp.stack([st[:n_state, lanes_of(k)] for k in range(tiles)])
        lax.fori_loop(0, tokens // GROUP, ahead, start)

        def behind(i, carry):
            later, rate = carry
            base = tokens - GROUP - i * GROUP
            for s in reversed(range(GROUP)):
                t = base + s
                bs = bx[t][None]
                state = cx[t][None] * row(gg, t, n_state) + later
                later = dec[t] * state
                weighted = later * hs[t]
                rate = rate + weighted * row(dl, t, n_state)
                one, two = state * bs, weighted * rates
                fold = slice(s * SUB, (s + 1) * SUB)
                csp[:, fold, :] = sum(one[:, h : h + SUB] for h in range(0, n_state, SUB))
                awp[:, fold, :] = sum(two[:, h : h + SUB] for h in range(0, n_state, SUB))
                accb[t] += jnp.sum(state * row(uu, t, n_state), axis=0)
            rows = pl.ds(pl.multiple_of(base, GROUP), GROUP)
            coeff = csp[:, pl.ds(0, GROUP, stride=SUB), :]
            weigh = awp[:, pl.ds(0, GROUP, stride=SUB), :]
            for s in range(1, SUB):
                coeff = coeff + csp[:, pl.ds(s, GROUP, stride=SUB), :]
                weigh = weigh + awp[:, pl.ds(s, GROUP, stride=SUB), :]
            gi[:, rows, :] = dl[:, rows, :] * coeff
            gs[:, rows, :] = xx[:, rows, :] * coeff + LN2 * weigh
            return later, rate

        last = jnp.stack([st[n_state : 2 * n_state, lanes_of(k)] for k in range(tiles)])
        _, rate = lax.fori_loop(
            0, tokens // GROUP, behind, (last, jnp.zeros(state_shape, F32))
        )
        for k in range(tiles):
            lanes = pl.ds(pl.multiple_of(b * block + k * LANES, LANES), LANES)
            gi_ref[:, lanes] = gi[k].astype(gi_ref.dtype)
            gs_ref[:, lanes] = gs[k].astype(gs_ref.dtype)
            st[:n_state, lanes_of(k)] = -rate[k]
        for j in range(owners):
            dest = b * owners + j
            out3[dest] = st[:n_state, j * width : (j + 1) * width]

            @pl.when(dest != me)
            def _():
                copy(*third, dest, me).start()

        return 0

    lax.fori_loop(0, blocks, differentiate, 0)
    in3[me] = out3[me]
    lane_sums(accb, gb_ref, tokens, n_state)
    lane_sums(accc, gc_ref, tokens, n_state)
    arrived(third)
    gr_ref[...] = lax.fori_loop(0, n, lambda d, total: total + in3[d], blank)
    for refs in (first, second, third):
        loop(1, n, lambda k: copy(*refs, lax.rem(me + k, n), me).wait_send())


def shards(n, inputs, step_sizes, cotangent, input_coeffs, output_coeffs, decay_rates):
    n_state, channels = decay_rates.shape
    tokens = inputs.shape[0]
    width = channels // n
    block = max(TILES * LANES, width)
    tiles = block // LANES
    wide = pltpu.VMEM((tokens, n_state, LANES), F32)
    rows = pltpu.VMEM((tiles, tokens, LANES), F32)
    states = pltpu.VMEM((tokens, tiles, n_state, LANES), F32)
    fold = pltpu.VMEM((tiles, GROUP * SUB, LANES), F32)
    vmem = pl.BlockSpec(memory_space=pltpu.VMEM)
    dma = pltpu.SemaphoreType.DMA((n,))
    head_rows = 2 * n_state + SUB
    slots = lambda count: [pltpu.VMEM((n, count, width), F32)] * 2
    return pl.pallas_call(
        partial(whole_kernel, n, block),
        name="whole",
        in_specs=[vmem] * 6,
        out_specs=[vmem] * 5,
        out_shape=[
            jax.ShapeDtypeStruct((tokens, channels), jnp.bfloat16),
            jax.ShapeDtypeStruct((tokens, channels), jnp.bfloat16),
            jax.ShapeDtypeStruct((n_state, tokens), F32),
            jax.ShapeDtypeStruct((n_state, tokens), F32),
            jax.ShapeDtypeStruct((n_state, width), F32),
        ],
        scratch_shapes=[
            wide, wide, rows, rows, rows, rows,
            pltpu.VMEM((tiles, n_state, LANES), F32),
            pltpu.VMEM((head_rows, block), F32),
            states, states, wide, wide, fold, fold, rows, rows,
            *slots(head_rows), *slots(2 * n_state), *slots(n_state),
            dma, dma, dma, dma, dma, dma,
        ],
        compiler_params=pltpu.CompilerParams(
            collective_id=0, has_side_effects=True, vmem_limit_bytes=60 * 1024 * 1024
        ),
    )(inputs, step_sizes, cotangent, input_coeffs, output_coeffs, decay_rates)


def solution(mesh):
    placed = (P("seq", None), P("seq", None), P("seq", None), P(None, "seq"), P(None, "seq"), P())
    return jax.shard_map(
        partial(shards, mesh.shape["seq"]),
        mesh=mesh,
        in_specs=placed,
        out_specs=(P("seq", None), P("seq", None), P(None, "seq"), P(None, "seq"), P(None, "seq")),
        check_vma=False,
    )
```

```python
from functools import partial
import math

import jax
import jax.numpy as jnp
from jax import lax
from jax.experimental import pallas as pl
from jax.experimental.pallas import tpu as pltpu
from jax.sharding import PartitionSpec as P

LANES = 128
SUB = 8
TILES = 4
GROUP = 8
LOG2E = math.log2(math.e)
LN2 = math.log(2.0)
F32 = jnp.float32
MESH = pl.DeviceIdType.MESH


def expand(coef_ref, wide, tokens, n_state):
    for t in range(tokens):
        wide[t] = jnp.broadcast_to(coef_ref[:, t : t + 1], (n_state, LANES))


def row(ref, t, n_state):
    return ref[:, pl.ds(t, n_state, stride=0), :]


def lanes_of(k):
    return slice(k * LANES, (k + 1) * LANES)


def loop(start, stop, body):
    def step(k, _):
        body(k)
        return 0

    lax.fori_loop(start, stop, step, 0)


def lane_sums(acc, out_ref, tokens, n_state):
    lane = lax.broadcasted_iota(jnp.int32, (n_state, tokens), 1)
    total = jnp.zeros((n_state, tokens), F32)
    for t in range(tokens):
        total = jnp.where(lane == t, jnp.sum(acc[t], axis=1, keepdims=True), total)
    out_ref[...] = total


def whole_kernel(
    n, block,
    x_ref, d_ref, g_ref, b_ref, c_ref, a_ref,
    gi_ref, gs_ref, gb_ref, gc_ref, gr_ref,
    bx, cx, dl, xx, uu, gg, rt, st, hs, dec, accb, accc, csp, awp, gi, gs,
    out1, in1, out2, in2, out3, in3, send1, recv1, send2, recv2, send3, recv3,
):
    me = lax.axis_index("seq")
    tokens, channels = x_ref.shape
    n_state = a_ref.shape[0]
    tiles, width = block // LANES, channels // n
    blocks, owners = channels // block, block // width
    home = me // owners
    barrier = pltpu.get_barrier_semaphore()

    def tell(k):
        pl.semaphore_signal(barrier, inc=1, device_id=(lax.rem(me + k, n),), device_id_type=MESH)

    def copy(src, dst, send_sem, recv_sem, dest, slot):
        return pltpu.make_async_remote_copy(
            src_ref=src.at[dest],
            dst_ref=dst.at[slot],
            send_sem=send_sem.at[dest],
            recv_sem=recv_sem.at[slot],
            device_id=(dest,),
            device_id_type=MESH,
        )

    first = (out1, in1, send1, recv1)
    second = (out2, in2, send2, recv2)
    third = (out3, in3, send3, recv3)

    def stage(b):
        for k in range(tiles):
            lanes = pl.ds(pl.multiple_of(b * block + k * LANES, LANES), LANES)
            delta = d_ref[:, lanes].astype(F32)
            x = x_ref[:, lanes].astype(F32)
            dl[k] = delta
            xx[k] = x
            uu[k] = delta * x
            gg[k] = g_ref[:, lanes].astype(F32)
            rt[k] = a_ref[:, lanes] * (-LOG2E)

    loop(1, n, tell)
    expand(b_ref, bx, tokens, n_state)
    expand(c_ref, cx, tokens, n_state)
    accb[...] = jnp.zeros_like(accb)
    accc[...] = jnp.zeros_like(accc)
    state_shape = (tiles, n_state, LANES)

    def summarize(order):
        b = lax.rem(home + 1 + order, blocks)
        stage(b)
        rates = rt[...]

        def group(i, carry):
            prod, end, back = carry
            for s in range(GROUP):
                t = i * GROUP + s
                decay = jnp.exp2(row(dl, t, n_state) * rates)
                end = decay * end + bx[t][None] * row(uu, t, n_state)
                prod = decay * prod
                back = back + prod * (cx[t][None] * row(gg, t, n_state))
            return prod, end, back

        zero = jnp.zeros(state_shape, F32)
        _, end, back = lax.fori_loop(
            0, tokens // GROUP, group, (jnp.ones(state_shape, F32), zero, zero)
        )
        for k in range(tiles):
            st[:n_state, lanes_of(k)] = end[k]
            st[n_state : 2 * n_state, lanes_of(k)] = back[k]
            st[2 * n_state :, lanes_of(k)] = jnp.broadcast_to(
                jnp.sum(dl[k], axis=0, keepdims=True), (1, LANES)
            )

        @pl.when(order == 0)
        def _():
            pl.semaphore_wait(barrier, n - 1)

        for j in range(owners):
            dest = b * owners + j
            out1[dest] = st[:, j * width : (j + 1) * width]

            @pl.when(dest != me)
            def _():
                copy(*first, dest, me).start()

    loop(0, blocks, summarize)
    in1[me] = out1[me]

    def arrived(refs):
        def wait(k):
            origin = lax.rem(me + n - k, n)
            copy(*refs, origin, origin).wait_recv()

        loop(1, n, wait)

    arrived(first)
    if width % LANES == 0:
        own = a_ref[:, pl.ds(pl.multiple_of(me * width, LANES), width)] * (-LOG2E)
    else:
        own = jnp.zeros((n_state, width), F32)
        for j in range(n):
            own = jnp.where(me == j, a_ref[:, j * width : (j + 1) * width] * (-LOG2E), own)

    def scan(i, carry):
        ahead, behind = carry
        d, e = i, n - 1 - i
        out2[d, :n_state, :] = ahead
        out2[e, n_state:, :] = behind
        ahead = jnp.exp2(own * in1[d, 2 * n_state : 2 * n_state + 1, :]) * ahead + in1[d, :n_state, :]
        behind = (
            jnp.exp2(own * in1[e, 2 * n_state : 2 * n_state + 1, :]) * behind
            + in1[e, n_state : 2 * n_state, :]
        )
        return ahead, behind

    blank = jnp.zeros((n_state, width), F32)
    lax.fori_loop(0, n, scan, (blank, blank), unroll=4)
    loop(1, n, lambda k: copy(*second, lax.rem(me + n - k, n), me).start())
    in2[me] = out2[me]

    def differentiate(order, _):
        b = lax.rem(home + order, blocks)
        stage(b)
        for j in range(owners):
            origin = b * owners + j

            @pl.when(origin != me)
            def _():
                copy(*second, origin, origin).wait_recv()

            st[: 2 * n_state, j * width : (j + 1) * width] = in2[origin]
        rates = rt[...]

        def ahead(i, hidden):
            for s in range(GROUP):
                t = i * GROUP + s
                decay = jnp.exp2(row(dl, t, n_state) * rates)
                dec[t] = decay
                hs[t] = hidden
                hidden = decay * hidden + bx[t][None] * row(uu, t, n_state)
                accc[t] += jnp.sum(row(gg, t, n_state) * hidden, axis=0)
            return hidden

        start = jnp.stack([st[:n_state, lanes_of(k)] for k in range(tiles)])
        lax.fori_loop(0, tokens // GROUP, ahead, start)

        def behind(i, carry):
            later, rate = carry
            base = tokens - GROUP - i * GROUP
            for s in reversed(range(GROUP)):
                t = base + s
                bs = bx[t][None]
                state = cx[t][None] * row(gg, t, n_state) + later
                later = dec[t] * state
                weighted = later * hs[t]
                rate = rate + weighted * row(dl, t, n_state)
                one, two = state * bs, weighted * rates
                fold = slice(s * SUB, (s + 1) * SUB)
                csp[:, fold, :] = sum(one[:, h : h + SUB] for h in range(0, n_state, SUB))
                awp[:, fold, :] = sum(two[:, h : h + SUB] for h in range(0, n_state, SUB))
                accb[t] += jnp.sum(state * row(uu, t, n_state), axis=0)
            rows = pl.ds(pl.multiple_of(base, GROUP), GROUP)
            coeff = csp[:, pl.ds(0, GROUP, stride=SUB), :]
            weigh = awp[:, pl.ds(0, GROUP, stride=SUB), :]
            for s in range(1, SUB):
                coeff = coeff + csp[:, pl.ds(s, GROUP, stride=SUB), :]
                weigh = weigh + awp[:, pl.ds(s, GROUP, stride=SUB), :]
            gi[:, rows, :] = dl[:, rows, :] * coeff
            gs[:, rows, :] = xx[:, rows, :] * coeff + LN2 * weigh
            return later, rate

        last = jnp.stack([st[n_state : 2 * n_state, lanes_of(k)] for k in range(tiles)])
        _, rate = lax.fori_loop(
            0, tokens // GROUP, behind, (last, jnp.zeros(state_shape, F32))
        )
        for k in range(tiles):
            lanes = pl.ds(pl.multiple_of(b * block + k * LANES, LANES), LANES)
            gi_ref[:, lanes] = gi[k].astype(gi_ref.dtype)
            gs_ref[:, lanes] = gs[k].astype(gs_ref.dtype)
            st[:n_state, lanes_of(k)] = -rate[k]
        for j in range(owners):
            dest = b * owners + j
            out3[dest] = st[:n_state, j * width : (j + 1) * width]

            @pl.when(dest != me)
            def _():
                copy(*third, dest, me).start()

        return 0

    lax.fori_loop(0, blocks, differentiate, 0)
    in3[me] = out3[me]
    lane_sums(accb, gb_ref, tokens, n_state)
    lane_sums(accc, gc_ref, tokens, n_state)
    arrived(third)
    gr_ref[...] = lax.fori_loop(0, n, lambda d, total: total + in3[d], blank)
    for refs in (first, second, third):
        loop(1, n, lambda k: copy(*refs, lax.rem(me + k, n), me).wait_send())


def shards(n, inputs, step_sizes, cotangent, input_coeffs, output_coeffs, decay_rates):
    n_state, channels = decay_rates.shape
    tokens = inputs.shape[0]
    width = channels // n
    block = max(TILES * LANES, width)
    tiles = block // LANES
    wide = pltpu.VMEM((tokens, n_state, LANES), F32)
    rows = pltpu.VMEM((tiles, tokens, LANES), F32)
    states = pltpu.VMEM((tokens, tiles, n_state, LANES), F32)
    fold = pltpu.VMEM((tiles, GROUP * SUB, LANES), F32)
    vmem = pl.BlockSpec(memory_space=pltpu.VMEM)
    dma = pltpu.SemaphoreType.DMA((n,))
    head_rows = 2 * n_state + 1
    slots = lambda count: [pltpu.VMEM((n, count, width), F32)] * 2
    return pl.pallas_call(
        partial(whole_kernel, n, block),
        name="whole",
        in_specs=[vmem] * 6,
        out_specs=[vmem] * 5,
        out_shape=[
            jax.ShapeDtypeStruct((tokens, channels), jnp.bfloat16),
            jax.ShapeDtypeStruct((tokens, channels), jnp.bfloat16),
            jax.ShapeDtypeStruct((n_state, tokens), F32),
            jax.ShapeDtypeStruct((n_state, tokens), F32),
            jax.ShapeDtypeStruct((n_state, width), F32),
        ],
        scratch_shapes=[
            wide, wide, rows, rows, rows, rows,
            pltpu.VMEM((tiles, n_state, LANES), F32),
            pltpu.VMEM((head_rows, block), F32),
            states, states, wide, wide, fold, fold, rows, rows,
            *slots(head_rows), *slots(2 * n_state), *slots(n_state),
            dma, dma, dma, dma, dma, dma,
        ],
        compiler_params=pltpu.CompilerParams(
            collective_id=0, has_side_effects=True, vmem_limit_bytes=60 * 1024 * 1024
        ),
    )(inputs, step_sizes, cotangent, input_coeffs, output_coeffs, decay_rates)


def solution(mesh):
    placed = (P("seq", None), P("seq", None), P("seq", None), P(None, "seq"), P(None, "seq"), P())
    return jax.shard_map(
        partial(shards, mesh.shape["seq"]),
        mesh=mesh,
        in_specs=placed,
        out_specs=(P("seq", None), P("seq", None), P(None, "seq"), P(None, "seq"), P(None, "seq")),
        check_vma=False,
    )
```
